32 devices in a mesh: aux: 8 (over z, x), row: 4 (over y, core).
Axes of the slice: x: 2, y: 2, z: 4, core: 2. Of those that a mesh axis runs over, the one named last changes fastest.
Arguments:
- slabs: bfloat16 [64, 400, 2048], P('aux', None, 'row'), may hold values from -0.47265625 to 0.47265625
- significant: int32 [64, 32], P('aux'), may hold values from 0 to 1, as said below
Outputs:
- exchange: float32 [2048, 2048], P('row', 'aux')
The draws below stay inside these ranges and needn't reach their ends.
Inputs may be any that keep to these rules, and one draw needn't show every extreme that they name: `significant`: each entry is 0 or 1; the share of ones differs between the auxiliary functions of different devices.
All inputs are finite; a program needn't handle non-finite values.
Results may differ from the reference program's by a relative error of at most 0.0003.
Values may be sent and summed in bfloat16 or wider, within the bound.
A program may use at most 64 MiB of HBM per device.

```python
import jax
import jax.numpy as jnp
from jax import lax

NBF = 2048
NOCC = 400
BS = 64
AUX_DEV = 8
NAUXW = 64
NBLK = 32


def draw_significant(key, part):
    first_key, second_key = jax.random.split(jax.random.fold_in(key, 11))
    groups = NAUXW // AUX_DEV
    levels = jax.random.randint(first_key, (groups, 1, 1), 3, 19)
    levels = jnp.broadcast_to(levels, (groups, AUX_DEV, NBLK)).reshape(NAUXW, NBLK)
    rolled = jax.random.randint(second_key, (NAUXW, NBLK), 0, 20)
    return (rolled < levels).astype(jnp.int32)


def block_levels(own_key, extent, cuts, low, largest):
    def one(position, blocks):
        draws = jax.random.uniform(jax.random.fold_in(jax.random.fold_in(own_key, 6), position), (blocks,), jnp.float32, low / len(cuts), largest / len(cuts))
        return jnp.repeat(jnp.exp(draws), extent[position] // blocks).reshape((-1,) + (1,) * (len(extent) - position - 1))

    level = one(*cuts[0])
    for cut in cuts[1:]:
        level = level * one(*cut)
    return level


def scatter_about(rng, extent, scale, most, cuts=(), held_as=jnp.bfloat16):
    level = block_levels(rng, extent, cuts, -0.22, 0.18) if cuts else 1.0
    entries = jax.random.normal(rng, extent, jnp.float32) * scale * level
    return jnp.minimum(jnp.maximum(entries, -most), most).astype(held_as)


def setup_inputs(seed: int = 0) -> dict:
    key_of = jax.random.split(jax.random.key(seed), 3)
    return {
        "slabs": scatter_about(key_of[0], (NAUXW, NOCC, NBF), ((NAUXW * NOCC) ** -0.25), 0.47265625, ((0, 8), (2, 4))),
        "significant": draw_significant(jax.random.fold_in(key_of[2], 71), 0),
    }


def reference(slabs, significant):
    block_of = lax.broadcasted_iota(jnp.int32, (NBLK, NBF), 1) // BS
    block_id = lax.broadcasted_iota(jnp.int32, (NBLK, NBF), 0)
    expand_table = (block_of == block_id).astype(jnp.float32)
    column_mask = jnp.dot(significant.astype(jnp.float32), expand_table).astype(jnp.bfloat16)
    masked = (slabs * column_mask[:, None, :]).reshape(NAUXW * NOCC, NBF)
    return lax.dot_general(masked, masked, (((0,), (0,)), ((), ())), preferred_element_type=jnp.float32)
```

```python
import functools

import jax
import jax.numpy as jnp
from jax import lax
from jax.experimental import pallas as pl
from jax.experimental.pallas import tpu as pltpu
from jax.sharding import PartitionSpec as P

BS = 64
LANES = 128
SUB = 128
LAG = 3
CHUNKS = 2
SUBS = 4
OWN_CHUNK = (0, 0, 1, 1, 1)
OWN_ROW = ((0, 2, 1, 0, 3), (2, 1, 3, 2, 0))


def plain(slabs, significant):
    aux_here, occupied, rows_here = slabs.shape
    blocks_here = rows_here // BS
    first_block = lax.axis_index("row") * blocks_here
    local_mask = lax.dynamic_slice_in_dim(significant, first_block, blocks_here, 1).astype(
        jnp.float32
    )
    block_of = lax.broadcasted_iota(jnp.int32, (blocks_here, rows_here), 1) // BS
    block_id = lax.broadcasted_iota(jnp.int32, (blocks_here, rows_here), 0)
    expand_table = (block_of == block_id).astype(jnp.float32)
    column_mask = jnp.dot(local_mask, expand_table).astype(jnp.bfloat16)
    masked = (slabs * column_mask[:, None, :]).reshape(aux_here * occupied, rows_here)
    partial_rows = lax.dot_general(
        masked,
        lax.all_gather(masked, "row", axis=1, tiled=True),
        (((0,), (0,)), ((), ())),
        preferred_element_type=jnp.float32,
    )
    return lax.psum_scatter(partial_rows, "aux", scatter_dimension=1, tiled=True)


def kernel(n_aux, n_row, occupied, slab_hbm, sig, out_ref, g, gy, lhs_t, mk, mkc, mask_ref, psd, pso, psc,
           xr, zb, zlo, zhi, mr, own_sem, psend, precv, ysend, yrecv, fsend, frecv, xsend, xrecv,
           zsend, zlo_sem, zhi_sem, msend, mrecv, go):
    depth = slab_hbm.shape[0]
    half = depth // 2
    aux_here = depth // occupied
    width = CHUNKS * LANES
    a, r = lax.axis_index("aux"), lax.axis_index("row")
    z, x = a // 2, a % 2
    last = n_aux // 2 - 1
    y, c = r // 2, r % 2
    partner = y * 2 + (1 - c)
    across = (1 - y) * 2 + c
    beside = z * 2 + (1 - x)
    over = ((1 - y) * 2 + (1 - y), (1 - y) * 2 + y)
    direct = jnp.where(c == y, 1, 0)
    sent = 1 - direct

    barrier = pltpu.get_barrier_semaphore()
    for there in ({"row": partner}, {"row": across}, {"aux": beside},
                  {"aux": lax.rem(a + 2, n_aux)}, {"aux": lax.rem(a + n_aux - 2, n_aux)}):
        pl.semaphore_signal(barrier, inc=1, device_id=there, device_id_type=pl.DeviceIdType.MESH)
    mirrored = z != r

    @pl.when(mirrored)
    def _():
        for q in range(2):
            pl.semaphore_signal(barrier, inc=1, device_id={"aux": r * 2 + q, "row": z},
                                device_id_type=pl.DeviceIdType.MESH)

    def lanes(h, j):
        return pl.ds(pl.multiple_of(h * width + j * LANES, LANES), LANES)

    def piece(j, h):
        return slab_hbm.at[:, lanes(h, j)]

    def remote(src, dst, send, recv, there):
        return pltpu.make_async_remote_copy(
            src_ref=src, dst_ref=dst, send_sem=send, recv_sem=recv, device_id=there,
            device_id_type=pl.DeviceIdType.MESH,
        )

    both = [(j, h) for j in range(CHUNKS) for h in range(2)]
    own = {w: pltpu.make_async_copy(piece(*w), g.at[(0,) + w], own_sem.at[w]) for w in both}
    for w in both:
        own[w].start()

    low_lanes = lax.broadcasted_iota(jnp.int32, (16, LANES), 1) < BS
    for q in range(aux_here):
        for d in range(n_row):
            for h in range(2):
                for j in range(CHUNKS):
                    b = (d * 2 * width + h * width + j * LANES) // BS
                    tile = jnp.where(low_lanes, sig[q, b], sig[q, b + 1])
                    mask_ref[d, h, j, q] = tile.astype(jnp.float32).astype(jnp.bfloat16)

    pl.semaphore_wait(barrier, jnp.where(mirrored, 7, 5))

    def side(i):
        return x if i else 1 - x

    def y_copy(j, i):
        first = pl.multiple_of((1 - y) * half, 16)
        return remote(slab_hbm.at[pl.ds(first, half), lanes(side(i), j)], gy.at[sent, j, i],
                      ysend.at[j, i], yrecv.at[j, i], {"row": across})

    def f_copy(q, j, i):
        return remote(gy.at[q, j, i], gy.at[q, j, i], fsend.at[j, i], frecv.at[j, i], {"row": partner})

    to_p = {w: remote(piece(*w), g.at[(1,) + w], psend.at[w], precv.at[w], {"row": partner}) for w in both}

    @pl.when(c == y)
    def _():
        for w in both:
            y_copy(*w).start()

    for w in both:
        to_p[w].start()

    def apply(raw, mask):
        return (raw.reshape(-1, occupied // 16, 16, LANES) * mask[:, None]).reshape(raw.shape)

    OWN, PAIR, FIRST, SECOND = range(4)
    count = (len(OWN_CHUNK), SUBS, CHUNKS * SUBS, CHUNKS * SUBS)
    base = [sum(count[:k]) for k in range(4)]
    dest = (r, partner) + over

    def rows_of(s):
        return pl.ds(s * SUB, SUB) if isinstance(s, int) else pl.ds(pl.multiple_of(s * SUB, SUB), SUB)

    def partial_tile(kind, i, there):
        if kind == OWN:
            s = jnp.where((x if not there else 1 - x) == 0, OWN_ROW[0][i], OWN_ROW[1][i])
            return psd.at[OWN_CHUNK[i], 1 - x if there else x, rows_of(s)]
        if kind == PAIR:
            return pso.at[1 - x if there else x, rows_of(i)]
        return psc.at[kind - FIRST, i // SUBS, 0 if there else 1, rows_of(i % SUBS)]

    def x_copy(kind, i):
        e = base[kind] + i
        return remote(partial_tile(kind, i, True), xr.at[e], xsend.at[e], xrecv.at[e], {"aux": beside})

    def z_copy(kind, i, up):
        e = base[kind] + i
        land, sem = (zlo, zlo_sem) if up else (zhi, zhi_sem)
        return remote(zb.at[e], land.at[e], zsend.at[e], sem.at[e],
                      {"aux": jnp.minimum(a + 2, n_aux - 1) if up else jnp.maximum(a - 2, 0)})

    def m_copy(kind, i):
        e = base[kind] + i
        if kind == OWN:
            slot = 0 if i == 1 else 1
            return remote(zb.at[e], mr.at[slot, 0], msend.at[slot, 0], mrecv.at[slot, 0], {"aux": beside})
        s = i % SUBS
        j = (s + c) % 2 if kind == PAIR else i // SUBS
        to = x * CHUNKS + j
        return remote(zb.at[e], mr.at[s % CHUNKS, to], msend.at[0 if kind == PAIR else i // SUBS, s],
                      mrecv.at[s % CHUNKS, to], {"aux": r * 2 + s // CHUNKS, "row": z})

    def sum_x(kind, i):
        e, d = base[kind] + i, dest[kind]
        x_copy(kind, i).wait_recv()
        zb[e] = partial_tile(kind, i, False)[...] + xr[e]
        pl.when((z == 0) & (d > 0))(lambda: z_copy(kind, i, True).start())
        pl.when((z == last) & (d < last))(lambda: z_copy(kind, i, False).start())

    def finish(kind, i):
        e = base[kind] + i
        if kind == OWN:
            j = OWN_CHUNK[i]
            for side_x in range(2):
                @pl.when(x == side_x)
                def _():
                    s = OWN_ROW[side_x][i]
                    out_ref[s * SUB:(s + 1) * SUB, j * LANES:(j + 1) * LANES] = zb[e]
                    if i == 3:
                        t = side_x * CHUNKS + j
                        u = (s % CHUNKS) * LANES
                        out_ref[t * SUB:(t + 1) * SUB, u:u + LANES] = zb[e].T
            if i in (1, 4):
                m_copy(kind, i).start()
        elif kind == PAIR:
            m_copy(kind, i).start()
            for core in range(2):
                @pl.when(c == core)
                def _():
                    j = (i + core) % 2
                    out_ref[i * SUB:(i + 1) * SUB, j * LANES:(j + 1) * LANES] = zb[e]
        else:
            m_copy(kind, i).start()

    def sum_z(kind, i):
        e, d = base[kind] + i, dest[kind]

        @pl.when((z > 0) & (z <= d))
        def _():
            z_copy(kind, i, True).wait_recv()
            zb[e] += zlo[e]

        @pl.when((z < last) & (z >= d))
        def _():
            z_copy(kind, i, False).wait_recv()
            zb[e] += zhi[e]

        pl.when((z > 0) & (z < d))(lambda: z_copy(kind, i, True).start())
        pl.when((z < last) & (z > d))(lambda: z_copy(kind, i, False).start())
        pl.when(z == d)(lambda: finish(kind, i))

    hops = [jnp.where(z < d, z, jnp.where(z > d, last - z, jnp.maximum(d, last - d))) for d in dest]
    line = []

    def advance(job):
        if job is not None:
            sum_x(*job)
        line.append(job)
        for hop in range(1, last + 1):
            due = len(line) - LAG * hop
            if due >= 0 and line[due] is not None:
                pl.when(hops[line[due][0]] == hop)(functools.partial(sum_z, *line[due]))

    def drain(steps):
        for _ in range(steps):
            advance(None)

    def pull(q, j, i):
        @pl.when(direct == q)
        def _():
            remote(gy.at[q, j, i], gy.at[q, j, i], ysend.at[j, i], yrecv.at[j, i], {"row": across}).wait_recv()
            f_copy(q, j, i).start()

    def product(q, j, i):
        pl.when(direct != q)(lambda: f_copy(q, j, i).wait_recv())
        here = half // occupied
        mkc[...] = apply(gy[q, j, i], mask_ref[over[q], side(i), j, pl.ds(y * here, here)])
        for s in range(0, SUBS, 2):
            part = slice(s * SUB, (s + 2) * SUB)
            psc[q, j, i, part, :] = jnp.dot(lhs_t[y, part, :], mkc[...], preferred_element_type=jnp.float32)
        if i == 0:
            for s in range(SUBS):
                x_copy(FIRST + q, j * SUBS + s).start()

    for j, h in both:
        own[j, h].wait()
        mk[j, :, h * LANES:(h + 1) * LANES] = apply(g[0, j, h], mask_ref[r, h, j])
        for e in range(2):
            t = h * CHUNKS + j
            lhs_t[e, t * LANES:(t + 1) * LANES, :] = mk[j, e * half:(e + 1) * half, h * LANES:(h + 1) * LANES].T
    for j in range(CHUNKS):
        for s in range(0, SUBS, 2):
            part = slice(s * SUB, (s + 2) * SUB)
            acc = jnp.dot(lhs_t[0, part, :], mk[j, :half, :], preferred_element_type=jnp.float32)
            acc += jnp.dot(lhs_t[1, part, :], mk[j, half:, :], preferred_element_type=jnp.float32)
            psd[j, 0, part, :] = acc[:, :LANES]
            psd[j, 1, part, :] = acc[:, LANES:]
        for i in range(len(OWN_CHUNK)):
            if OWN_CHUNK[i] == j:
                x_copy(OWN, i).start()

    @pl.when(c == y)
    def _():
        y_copy(0, 0).wait_send()
        pl.semaphore_signal(go, inc=1, device_id={"row": partner}, device_id_type=pl.DeviceIdType.MESH)

    @pl.when(c != y)
    def _():
        pl.semaphore_wait(go, 1)
        for w in both:
            y_copy(*w).start()

    pull(0, 0, 0)
    for j, h in both:
        to_p[j, h].wait_recv()
        mk[j, :, h * LANES:(h + 1) * LANES] = apply(g[1, j, h], mask_ref[partner, h, j])
    for s in range(SUBS):
        part = slice(s * SUB, (s + 1) * SUB)
        j = (s + c) % 2
        acc = jnp.dot(lhs_t[0, part, :], mk[j, :half, :], preferred_element_type=jnp.float32)
        acc += jnp.dot(lhs_t[1, part, :], mk[j, half:, :], preferred_element_type=jnp.float32)
        pso[0, part, :] = acc[:, :LANES]
        pso[1, part, :] = acc[:, LANES:]
        x_copy(PAIR, s).start()
    product(0, 0, 0)

    for i in range(len(OWN_CHUNK)):
        advance((OWN, i))
    for i in range(SUBS):
        advance((PAIR, i))

    def chunk(q, j):
        for s in range(SUBS):
            advance((FIRST + q, j * SUBS + s))

    order = [(q, j) for j in range(CHUNKS) for q in range(2)]
    for n, (q, j) in enumerate(order):
        if n + 1 < len(order):
            pull(*order[n + 1], 0)
            pull(q, j, 1)
            product(*order[n + 1], 0)
        else:
            pull(q, j, 1)
        product(q, j, 1)
        chunk(q, j)
    drain(LAG * last)

    @pl.when(z == r)
    def _():
        for slot in range(2):
            m_copy(OWN, 1 + 3 * slot).wait_recv()
            for side_x in range(2):
                @pl.when(x == side_x)
                def _():
                    s, t = OWN_ROW[1 - side_x][1 + 3 * slot], (1 - side_x) * CHUNKS + OWN_CHUNK[1 + 3 * slot]
                    u = (s % CHUNKS) * LANES
                    out_ref[t * SUB:(t + 1) * SUB, u:u + LANES] = mr[slot, 0].T
        for slot in range(2):
            m_copy(OWN, 1 + 3 * slot).wait_send()

    def landed(j, t):
        remote(mr.at[j, t], mr.at[j, t], msend.at[j, t], mrecv.at[j, t], {"aux": r * 2, "row": z}).wait_recv()

    for core in range(2):
        @pl.when((z == partner) & (c == core))
        def _():
            for t in range(SUBS):
                j = 1 - (t + core) % 2
                landed(j, t)
                out_ref[t * SUB:(t + 1) * SUB, j * LANES:(j + 1) * LANES] = mr[j, t].T
            for s in range(SUBS):
                m_copy(PAIR, s).wait_send()

    for q in range(2):
        @pl.when(z == over[q])
        def _():
            for first in range(CHUNKS):
                for t in range(first, SUBS, CHUNKS):
                    for j in range(CHUNKS):
                        landed(j, t)
                        out_ref[t * SUB:(t + 1) * SUB, j * LANES:(j + 1) * LANES] = (
                            zb[base[FIRST + q] + j * SUBS + t] + mr[j, t].T)
            for i in range(CHUNKS * SUBS):
                m_copy(FIRST + q, i).wait_send()

    pl.when(c != y)(lambda: y_copy(0, 0).wait_send())
    for w in both:
        if w != (0, 0):
            y_copy(*w).wait_send()
        to_p[w].wait_send()
        f_copy(direct, *w).wait_send()
    for kind in range(4):
        for i in range(count[kind]):
            x_copy(kind, i).wait_send()
            pl.when(z != dest[kind])(lambda: z_copy(kind, i, True).wait_send())


def solution(mesh):
    n_aux, n_row = mesh.shape["aux"], mesh.shape["row"]

    def local(slabs, significant):
        aux_here, occupied, rows = slabs.shape
        nbf = rows * n_row
        cols = nbf // n_aux
        fits = (n_row == 4 and n_aux == 2 * n_row and cols == CHUNKS * LANES and rows == SUBS * SUB
                and occupied % 16 == 0 and aux_here % 2 == 0 and LANES == 2 * BS)
        if not fits:
            return plain(slabs, significant)
        depth = aux_here * occupied
        items = len(OWN_CHUNK) + SUBS + 2 * CHUNKS * SUBS
        dma = pltpu.SemaphoreType.DMA
        tile = pltpu.VMEM((items, SUB, LANES), jnp.float32)
        return pl.pallas_call(
            functools.partial(kernel, n_aux, n_row, occupied),
            out_shape=jax.ShapeDtypeStruct((rows, cols), jnp.float32),
            in_specs=[pl.BlockSpec(memory_space=pl.ANY), pl.BlockSpec(memory_space=pltpu.SMEM)],
            out_specs=pl.BlockSpec(memory_space=pltpu.VMEM),
            scratch_shapes=[
                pltpu.VMEM((2, CHUNKS, 2, depth, LANES), jnp.bfloat16),
                pltpu.VMEM((2, CHUNKS, 2, depth // 2, LANES), jnp.bfloat16),
                pltpu.VMEM((2, rows, depth // 2), jnp.bfloat16),
                pltpu.VMEM((CHUNKS, depth, 2 * LANES), jnp.bfloat16),
                pltpu.VMEM((depth // 2, LANES), jnp.bfloat16),
                pltpu.VMEM((n_row, 2, CHUNKS, aux_here, 16, LANES), jnp.bfloat16),
                pltpu.VMEM((CHUNKS, 2, rows, LANES), jnp.float32),
                pltpu.VMEM((2, rows, LANES), jnp.float32),
                pltpu.VMEM((2, CHUNKS, 2, rows, LANES), jnp.float32),
            ]
            + [tile] * 4
            + [pltpu.VMEM((CHUNKS, SUBS, SUB, LANES), jnp.float32)]
            + [dma((CHUNKS, 2))] * 7
            + [dma((items,))] * 5
            + [dma((CHUNKS, SUBS))] * 2
            + [pltpu.SemaphoreType.REGULAR],
            compiler_params=pltpu.CompilerParams(
                collective_id=0, has_side_effects=True, vmem_limit_bytes=60 * 2**20
            ),
            cost_estimate=pl.CostEstimate(
                flops=2 * rows * nbf * depth, bytes_accessed=2 * depth * rows, transcendentals=0
            ),
        )(slabs.reshape(depth, rows), significant)

    return jax.shard_map(
        local,
        mesh=mesh,
        in_specs=(P("aux", None, "row"), P("aux", None)),
        out_specs=P("row", "aux"),
        check_vma=False,
    )
```

```python
import functools

import jax
import jax.numpy as jnp
from jax import lax
from jax.experimental import pallas as pl
from jax.experimental.pallas import tpu as pltpu
from jax.sharding import PartitionSpec as P

BS = 64
LANES = 128
SUB = 128
CHUNKS = 2
OWN, PAIR, FIRST, SECOND, PIECES, PULL = range(6)
TURNED = (
    (2, 1), (2, 2), (2, 3), (2, 5), (2, 7), (3, 1), (3, 2), (3, 4), (3, 5), (3, 7),
)
HELD = (
    (2, 1), (2, 2), (2, 5), (2, 6), (3, 2), (3, 4), (3, 5), (3, 7),
)
ORDER = (
    (0, 0, 0), (0, 0, 1), (0, 1, 0), (0, 1, 1), (0, 2, 0), (0, 1, 2), (0, 0, 2), (0, 0, 3), (0, 3, 0), (0, 4, 0),
    (1, 0, 0), (1, 1, 0), (0, 2, 1), (5, 0, 0), (5, 1, 0), (1, 2, 0), (4, 0, 0), (0, 3, 1), (4, 1, 0), (0, 3, 2),
    (5, 2, 0), (2, 0, 0), (2, 1, 0), (0, 4, 1), (2, 0, 1), (2, 3, 0), (4, 2, 0), (1, 0, 1), (0, 2, 2), (2, 2, 0),
    (1, 1, 1), (0, 3, 3), (2, 3, 1), (1, 3, 0), (5, 3, 0), (4, 3, 0), (2, 1, 1), (0, 4, 2), (3, 1, 0), (1, 2, 1),
    (2, 0, 2), (0, 1, 3), (2, 2, 1), (3, 0, 0), (1, 3, 1), (3, 3, 0), (5, 4, 0), (5, 5, 0), (3, 1, 1), (4, 4, 0),
    (3, 3, 1), (2, 3, 2), (1, 0, 2), (1, 1, 2), (3, 2, 0), (2, 0, 3), (4, 5, 0), (2, 5, 0), (2, 1, 2), (2, 2, 2),
    (2, 7, 0), (3, 0, 1), (2, 6, 0), (3, 2, 1), (2, 1, 3), (2, 4, 0), (3, 1, 2), (0, 4, 3), (2, 3, 3), (5, 6, 0),
    (4, 6, 0), (0, 2, 3), (2, 5, 1), (2, 2, 3), (2, 5, 2), (3, 4, 0), (2, 6, 1), (2, 7, 1), (2, 7, 2), (1, 3, 2),
    (1, 2, 2), (3, 5, 0), (3, 3, 2), (3, 6, 0), (3, 4, 1), (3, 7, 0), (2, 4, 1), (1, 1, 3), (3, 2, 2), (3, 5, 1),
    (3, 6, 1), (1, 0, 3), (2, 7, 3), (2, 6, 2), (2, 5, 3), (3, 4, 2), (2, 4, 2), (3, 7, 1), (3, 7, 2), (3, 0, 2),
    (3, 5, 2), (3, 6, 2), (3, 0, 3), (3, 1, 3), (2, 6, 3), (3, 3, 3), (1, 3, 3), (3, 2, 3), (3, 5, 3), (1, 2, 3),
    (2, 4, 3), (3, 7, 3), (3, 6, 3), (3, 4, 3),
)
FLAT = (
    (0, 0), (0, 2), (1, 2), (2, 1), (2, 4), (3, 0),
)
PAIRED = (
    (1, 1), (2, 0), (2, 2), (2, 3), (2, 6), (3, 1), (3, 2), (3, 5), (3, 7),
)
PAIR_SENT = (-1, -1, -1, -2)
SUBS = 4
OWN_CHUNK = (0, 0, 1, 1, 1)
OWN_ROW = ((0, 2, 1, 0, 3), (2, 1, 3, 2, 0))


def plain(slabs, significant):
    aux_here, occupied, rows_here = slabs.shape
    blocks_here = rows_here // BS
    first_block = lax.axis_index("row") * blocks_here
    local_mask = lax.dynamic_slice_in_dim(significant, first_block, blocks_here, 1).astype(
        jnp.float32
    )
    block_of = lax.broadcasted_iota(jnp.int32, (blocks_here, rows_here), 1) // BS
    block_id = lax.broadcasted_iota(jnp.int32, (blocks_here, rows_here), 0)
    expand_table = (block_of == block_id).astype(jnp.float32)
    column_mask = jnp.dot(local_mask, expand_table).astype(jnp.bfloat16)
    masked = (slabs * column_mask[:, None, :]).reshape(aux_here * occupied, rows_here)
    partial_rows = lax.dot_general(
        masked,
        lax.all_gather(masked, "row", axis=1, tiled=True),
        (((0,), (0,)), ((), ())),
        preferred_element_type=jnp.float32,
    )
    return lax.psum_scatter(partial_rows, "aux", scatter_dimension=1, tiled=True)


def kernel(n_aux, n_row, occupied, slab_hbm, sig, out_ref, g, gy, lhs_t, mk, mkc, mask_ref, psd, pso, psc,
           xr, zb, zl, nb, mr, own_sem, psend, precv, ysend, yrecv, fsend, frecv, xsend, xrecv,
           zsend, zrecv, nsend, nrecv, msend, mrecv, go):
    depth = slab_hbm.shape[0]
    half = depth // 2
    aux_here = depth // occupied
    width = CHUNKS * LANES
    a, r = lax.axis_index("aux"), lax.axis_index("row")
    z, x = a // 2, a % 2
    last = n_aux // 2 - 1
    y, c = r // 2, r % 2
    partner = y * 2 + (1 - c)
    across = (1 - y) * 2 + c
    beside = z * 2 + (1 - x)
    over = ((1 - y) * 2 + (1 - y), (1 - y) * 2 + y)
    direct = jnp.where(c == y, 1, 0)
    sent = 1 - direct

    barrier = pltpu.get_barrier_semaphore()
    for there in ({"row": partner}, {"row": across}, {"aux": beside},
                  *({"aux": lax.rem(a + 2 * n, n_aux)} for n in range(1, n_aux // 2))):
        pl.semaphore_signal(barrier, inc=1, device_id=there, device_id_type=pl.DeviceIdType.MESH)

    def greet(*theirs):
        for there in theirs:
            pl.semaphore_signal(barrier, inc=1, device_id=there, device_id_type=pl.DeviceIdType.MESH)

    pl.when(z != r)(lambda: greet(*({"aux": r * 2 + q, "row": z} for q in range(2))))

    @pl.when(z == r)
    def _():
        greet(*({"aux": r * 2 + q, "row": d} for q in range(2) for d in over))

    @pl.when((z != r) & (z != partner))
    def _():
        greet(*({"aux": z * 2 + q, "row": z} for q in range(2)))

    def lanes(h, j):
        return pl.ds(pl.multiple_of(h * width + j * LANES, LANES), LANES)

    def piece(j, h):
        return slab_hbm.at[:, lanes(h, j)]

    def remote(src, dst, send, recv, there):
        return pltpu.make_async_remote_copy(
            src_ref=src, dst_ref=dst, send_sem=send, recv_sem=recv, device_id=there,
            device_id_type=pl.DeviceIdType.MESH,
        )

    both = [(j, h) for j in range(CHUNKS) for h in range(2)]
    own = {w: pltpu.make_async_copy(piece(*w), g.at[(0,) + w], own_sem.at[w]) for w in both}
    for w in both:
        own[w].start()

    low_lanes = lax.broadcasted_iota(jnp.int32, (16, LANES), 1) < BS
    for q in range(aux_here):
        for d in range(n_row):
            for h in range(2):
                for j in range(CHUNKS):
                    b = (d * 2 * width + h * width + j * LANES) // BS
                    tile = jnp.where(low_lanes, sig[q, b], sig[q, b + 1])
                    mask_ref[d, h, j, q] = tile.astype(jnp.float32).astype(jnp.bfloat16)

    pl.semaphore_wait(barrier, jnp.where(z == partner, 8, 10))

    def side(i):
        return x if i else 1 - x

    def y_copy(j, i):
        first = pl.multiple_of((1 - y) * half, 16)
        return remote(slab_hbm.at[pl.ds(first, half), lanes(side(i), j)], gy.at[sent, j, i],
                      ysend.at[j, i], yrecv.at[j, i], {"row": across})

    def f_copy(q, j, i):
        return remote(gy.at[q, j, i], gy.at[q, j, i], fsend.at[j, i], frecv.at[j, i], {"row": partner})

    to_p = {w: remote(piece(*w), g.at[(1,) + w], psend.at[w], precv.at[w], {"row": partner}) for w in both}

    @pl.when(c == y)
    def _():
        for w in both:
            y_copy(*w).start()

    for w in both:
        to_p[w].start()

    def apply(raw, mask):
        return (raw.reshape(-1, occupied // 16, 16, LANES) * mask[:, None]).reshape(raw.shape)

    count = (len(OWN_CHUNK), SUBS, CHUNKS * SUBS, CHUNKS * SUBS)
    base = [sum(count[:k]) for k in range(4)]

    def turned(kind, i):
        return (kind, i) in TURNED

    def dest(kind, i):
        return r if kind == OWN or turned(kind, i) else partner if kind == PAIR else over[kind - FIRST]

    def rows_of(s):
        return pl.ds(s * SUB, SUB) if isinstance(s, int) else pl.ds(pl.multiple_of(s * SUB, SUB), SUB)

    def partial_tile(kind, i, there):
        if kind == OWN:
            s = jnp.where((x if not there else 1 - x) == 0, OWN_ROW[0][i], OWN_ROW[1][i])
            return psd.at[OWN_CHUNK[i], 1 - x if there else x, rows_of(s)]
        if kind == PAIR:
            return pso.at[1 - x if there else x, rows_of(i)]
        return psc.at[kind - FIRST, i // SUBS, 0 if there else 1, rows_of(i % SUBS)]

    def x_copy(kind, i):
        e = base[kind] + i
        return remote(partial_tile(kind, i, True), xr.at[e], xsend.at[e], xrecv.at[e], {"aux": beside})

    def parent(kind, i):
        d = dest(kind, i)
        near = jnp.where(z < d, z + 1, z - 1)
        if (kind, i) in FLAT:
            return d
        if (kind, i) in PAIRED:
            return jnp.where((d == 0) & (z == 2) | (d == last) & (z == 1), d, near)
        return near

    def z_copy(kind, i):
        e = base[kind] + i
        return remote(zb.at[e], zl.at[e, z], zsend.at[e], zrecv.at[e, z], {"aux": parent(kind, i) * 2 + x})

    def add_from(kind, i, child):
        e = base[kind] + i
        remote(zb.at[e], zl.at[e, child], zsend.at[e], zrecv.at[e, child], {"aux": beside}).wait_recv()
        zb[e] += zl[e, child]

    def level(kind, i):
        d = dest(kind, i)
        if (kind, i) in FLAT:
            return jnp.where(z == d, 1, 0)
        line = jnp.where(z < d, z, jnp.where(z > d, last - z, jnp.maximum(d, last - d)))
        if (kind, i) in PAIRED:
            inner = jnp.where((z == 0) | (z == last) | (jnp.abs(z - d) == 1), 0, 1)
            return jnp.where((d == 0) | (d == last), jnp.where(z == d, 2, inner), line)
        return line

    def m_copy(kind, i):
        e = base[kind] + i
        if kind == OWN:
            slot = 0 if i == 1 else 1
            return remote(zb.at[e], mr.at[slot, 0], msend.at[e], mrecv.at[slot, 0], {"aux": beside})
        s = i % SUBS
        j = (s + c) % 2 if kind == PAIR else i // SUBS
        to = x * CHUNKS + j
        return remote(zb.at[e], mr.at[s % CHUNKS, to], msend.at[e], mrecv.at[s % CHUNKS, to],
                      {"aux": r * 2 + s // CHUNKS, "row": partner if kind == PAIR else over[kind - FIRST]})

    def n_copy(kind, i):
        e = (kind - FIRST) * CHUNKS * SUBS + i
        return remote(zb.at[base[kind] + i], nb.at[e], nsend.at[e], nrecv.at[e], {"aux": over[kind - FIRST] * 2 + x})

    def sum_x(kind, i):
        e = base[kind] + i
        x_copy(kind, i).wait_recv()
        zb[e] = partial_tile(kind, i, False)[...] + xr[e]
        pl.when(level(kind, i) == 0)(lambda: z_copy(kind, i).start())

    def finish(kind, i, hop):
        e = base[kind] + i
        if kind == OWN:
            j = OWN_CHUNK[i]
            for side_x in range(2):
                @pl.when(x == side_x)
                def _():
                    s = OWN_ROW[side_x][i]
                    out_ref[s * SUB:(s + 1) * SUB, j * LANES:(j + 1) * LANES] = zb[e]
                    if i == 3:
                        t = side_x * CHUNKS + j
                        u = (s % CHUNKS) * LANES
                        out_ref[t * SUB:(t + 1) * SUB, u:u + LANES] = zb[e].T
            if i in (1, 4):
                m_copy(kind, i).start()
        elif kind == PAIR:
            m_copy(kind, i).start()
            for core in range(2):
                @pl.when(c == core)
                def _():
                    j = (i + core) % 2
                    out_ref[i * SUB:(i + 1) * SUB, j * LANES:(j + 1) * LANES] = zb[e]
        else:
            if turned(kind, i):
                n_copy(kind, i).start()
            if late[0] or (kind, i) not in HELD:
                m_copy(kind, i).start()
            else:
                held.append((kind, i, hop))

    def sum_z(kind, i, hop):
        d = dest(kind, i)
        if (kind, i) in FLAT:
            for away in range(1, last + 1):
                add_from(kind, i, lax.rem(z + away, last + 1))
        elif (kind, i) in PAIRED:
            ends = (d == 0) | (d == last)
            far = jnp.where(z == d, jnp.where(d == 0, 2, 1), jnp.where(d == 0, last, 0))
            pl.when(ends)(lambda: add_from(kind, i, far))
            pl.when(ends & (z == d))(lambda: add_from(kind, i, jnp.where(d == 0, 1, last - 1)))
            pl.when(~ends & (z > 0) & (z <= d))(lambda: add_from(kind, i, z - 1))
            pl.when(~ends & (z < last) & (z >= d))(lambda: add_from(kind, i, z + 1))
        else:
            pl.when((z > 0) & (z <= d))(lambda: add_from(kind, i, z - 1))
            pl.when((z < last) & (z >= d))(lambda: add_from(kind, i, z + 1))
        pl.when(z != d)(lambda: z_copy(kind, i).start())
        pl.when(z == d)(lambda: finish(kind, i, hop))

    late, held = [False], []

    def pull(q, j, i):
        @pl.when(direct == q)
        def _():
            remote(gy.at[q, j, i], gy.at[q, j, i], ysend.at[j, i], yrecv.at[j, i], {"row": across}).wait_recv()
            f_copy(q, j, i).start()

    def product(q, j, i):
        pl.when(direct != q)(lambda: f_copy(q, j, i).wait_recv())
        here = half // occupied
        mkc[...] = apply(gy[q, j, i], mask_ref[over[q], side(i), j, pl.ds(y * here, here)])
        for s in range(0, SUBS, 2):
            part = slice(s * SUB, (s + 2) * SUB)
            psc[q, j, i, part, :] = jnp.dot(lhs_t[y, part, :], mkc[...], preferred_element_type=jnp.float32)
        if i == 0:
            for s in range(SUBS):
                x_copy(FIRST + q, j * SUBS + s).start()

    for j, h in both:
        own[j, h].wait()
        mk[j, :, h * LANES:(h + 1) * LANES] = apply(g[0, j, h], mask_ref[r, h, j])
        for e in range(2):
            t = h * CHUNKS + j
            lhs_t[e, t * LANES:(t + 1) * LANES, :] = mk[j, e * half:(e + 1) * half, h * LANES:(h + 1) * LANES].T
    for j in range(CHUNKS):
        for s in range(0, SUBS, 2):
            part = slice(s * SUB, (s + 2) * SUB)
            acc = jnp.dot(lhs_t[0, part, :], mk[j, :half, :], preferred_element_type=jnp.float32)
            acc += jnp.dot(lhs_t[1, part, :], mk[j, half:, :], preferred_element_type=jnp.float32)
            psd[j, 0, part, :] = acc[:, :LANES]
            psd[j, 1, part, :] = acc[:, LANES:]
        for i in range(len(OWN_CHUNK)):
            if OWN_CHUNK[i] == j:
                x_copy(OWN, i).start()

    @pl.when(c == y)
    def _():
        y_copy(0, 0).wait_send()
        pl.semaphore_signal(go, inc=1, device_id={"row": partner}, device_id_type=pl.DeviceIdType.MESH)

    @pl.when(c != y)
    def _():
        pl.semaphore_wait(go, 1)
        for w in both:
            y_copy(*w).start()

    pull(0, 0, 0)
    for j, h in both:
        to_p[j, h].wait_recv()
        mk[j, :, h * LANES:(h + 1) * LANES] = apply(g[1, j, h], mask_ref[partner, h, j])
    for s in range(SUBS):
        part = slice(s * SUB, (s + 1) * SUB)
        j = (s + c) % 2
        acc = jnp.dot(lhs_t[0, part, :], mk[j, :half, :], preferred_element_type=jnp.float32)
        acc += jnp.dot(lhs_t[1, part, :], mk[j, half:, :], preferred_element_type=jnp.float32)
        pso[0, part, :] = acc[:, :LANES]
        pso[1, part, :] = acc[:, LANES:]
        if PAIR_SENT[s] == -1:
            x_copy(PAIR, s).start()
    product(0, 0, 0)
    for s in range(SUBS):
        if PAIR_SENT[s] == -2:
            x_copy(PAIR, s).start()

    order = [(q, j) for j in range(CHUNKS) for q in range(2)]

    groups = [(order[1], 0)]
    for n in range(len(order)):
        groups.append((order[n], 1))
        if n + 2 < len(order):
            groups.append((order[n + 2], 0))

    def step(n):
        product(*groups[n][0], groups[n][1])
        for p in range(SUBS):
            if PAIR_SENT[p] == n:
                x_copy(PAIR, p).start()

    def release():
        for kind, i, hop in held:
            d = dest(kind, i)
            pl.when((z == d) & (level(kind, i) == hop))(lambda: m_copy(kind, i).start())
        late[0] = True

    for kind, i, hop in ORDER:
        if kind == PULL:
            pull(*groups[i][0], groups[i][1])
        elif kind == PIECES:
            step(i)
            if i == len(groups) - 1:
                release()
        elif hop == 0:
            sum_x(kind, i)
        else:
            pl.when(level(kind, i) == hop)(functools.partial(sum_z, kind, i, hop))

    @pl.when(z == r)
    def _():
        for slot in range(2):
            m_copy(OWN, 1 + 3 * slot).wait_recv()
            for side_x in range(2):
                @pl.when(x == side_x)
                def _():
                    s, t = OWN_ROW[1 - side_x][1 + 3 * slot], (1 - side_x) * CHUNKS + OWN_CHUNK[1 + 3 * slot]
                    u = (s % CHUNKS) * LANES
                    out_ref[t * SUB:(t + 1) * SUB, u:u + LANES] = mr[slot, 0].T
        for slot in range(2):
            m_copy(OWN, 1 + 3 * slot).wait_send()

    def landed(j, t):
        remote(mr.at[j, t], mr.at[j, t], msend.at[0], mrecv.at[j, t], {"aux": r * 2, "row": z}).wait_recv()

    for core in range(2):
        @pl.when((z == partner) & (c == core))
        def _():
            for t in range(SUBS):
                j = 1 - (t + core) % 2
                landed(j, t)
                out_ref[t * SUB:(t + 1) * SUB, j * LANES:(j + 1) * LANES] = mr[j, t].T
            for s in range(SUBS):
                m_copy(PAIR, s).wait_send()

    for q in range(2):
        @pl.when(z == over[q])
        def _():
            for j_from in range(CHUNKS):
                for j in range(CHUNKS):
                    for t in range(j_from, SUBS, CHUNKS):
                        i = j * SUBS + t
                        if turned(FIRST + q, i):
                            n_copy(FIRST + q, i).wait_recv()
                            mine = nb.at[q * CHUNKS * SUBS + i]
                        else:
                            mine = zb.at[base[FIRST + q] + i]
                        landed(j, t)
                        out_ref[t * SUB:(t + 1) * SUB, j * LANES:(j + 1) * LANES] = mine[...] + mr[j, t].T

        for i in range(CHUNKS * SUBS):
            @pl.when(z == dest(FIRST + q, i))
            def _():
                m_copy(FIRST + q, i).wait_send()
                if turned(FIRST + q, i):
                    n_copy(FIRST + q, i).wait_send()

    pl.when(c != y)(lambda: y_copy(0, 0).wait_send())
    for w in both:
        if w != (0, 0):
            y_copy(*w).wait_send()
        to_p[w].wait_send()
        f_copy(direct, *w).wait_send()
    for kind in range(4):
        for i in range(count[kind]):
            x_copy(kind, i).wait_send()
            pl.when(z != dest(kind, i))(lambda: z_copy(kind, i).wait_send())


def solution(mesh):
    n_aux, n_row = mesh.shape["aux"], mesh.shape["row"]

    def local(slabs, significant):
        aux_here, occupied, rows = slabs.shape
        nbf = rows * n_row
        cols = nbf // n_aux
        fits = (n_row == 4 and n_aux == 2 * n_row and cols == CHUNKS * LANES and rows == SUBS * SUB
                and occupied % 16 == 0 and aux_here % 2 == 0 and LANES == 2 * BS)
        if not fits:
            return plain(slabs, significant)
        depth = aux_here * occupied
        items = len(OWN_CHUNK) + SUBS + 2 * CHUNKS * SUBS
        dma = pltpu.SemaphoreType.DMA
        tile = pltpu.VMEM((items, SUB, LANES), jnp.float32)
        return pl.pallas_call(
            functools.partial(kernel, n_aux, n_row, occupied),
            out_shape=jax.ShapeDtypeStruct((rows, cols), jnp.float32),
            in_specs=[pl.BlockSpec(memory_space=pl.ANY), pl.BlockSpec(memory_space=pltpu.SMEM)],
            out_specs=pl.BlockSpec(memory_space=pltpu.VMEM),
            scratch_shapes=[
                pltpu.VMEM((2, CHUNKS, 2, depth, LANES), jnp.bfloat16),
                pltpu.VMEM((2, CHUNKS, 2, depth // 2, LANES), jnp.bfloat16),
                pltpu.VMEM((2, rows, depth // 2), jnp.bfloat16),
                pltpu.VMEM((CHUNKS, depth, 2 * LANES), jnp.bfloat16),
                pltpu.VMEM((depth // 2, LANES), jnp.bfloat16),
                pltpu.VMEM((n_row, 2, CHUNKS, aux_here, 16, LANES), jnp.bfloat16),
                pltpu.VMEM((CHUNKS, 2, rows, LANES), jnp.float32),
                pltpu.VMEM((2, rows, LANES), jnp.float32),
                pltpu.VMEM((2, CHUNKS, 2, rows, LANES), jnp.float32),
            ]
            + [tile] * 2
            + [pltpu.VMEM((items, n_aux // 2, SUB, LANES), jnp.float32)]
            + [pltpu.VMEM((2 * CHUNKS * SUBS, SUB, LANES), jnp.float32)]
            + [pltpu.VMEM((CHUNKS, SUBS, SUB, LANES), jnp.float32)]
            + [dma((CHUNKS, 2))] * 7
            + [dma((items,))] * 3
            + [dma((items, n_aux // 2))]
            + [dma((2 * CHUNKS * SUBS,))] * 2
            + [dma((items,)), dma((CHUNKS, SUBS))]
            + [pltpu.SemaphoreType.REGULAR],
            compiler_params=pltpu.CompilerParams(
                collective_id=0, has_side_effects=True, vmem_limit_bytes=60 * 2**20
            ),
            cost_estimate=pl.CostEstimate(
                flops=2 * rows * nbf * depth, bytes_accessed=2 * depth * rows, transcendentals=0
            ),
        )(slabs.reshape(depth, rows), significant)

    return jax.shard_map(
        local,
        mesh=mesh,
        in_specs=(P("aux", None, "row"), P("aux", None)),
        out_specs=P("row", "aux"),
        check_vma=False,
    )
```

```python
import functools

import jax
import jax.numpy as jnp
from jax import lax
from jax.experimental import pallas as pl
from jax.experimental.pallas import tpu as pltpu
from jax.sharding import PartitionSpec as P

BS = 64
LANES = 128
SUB = 128
CHUNKS = 2
OWN, PAIR, FIRST, SECOND, PIECES, PULL = range(6)
TURNED = (
    (2, 1), (2, 2), (2, 3), (2, 5), (2, 7), (3, 1), (3, 2), (3, 4), (3, 7),
)
HELD = (
    (2, 1), (2, 2), (2, 5), (2, 6), (2, 7), (3, 2), (3, 4), (3, 6), (3, 7),
)
ORDER = (
    (0, 0, 0), (0, 1, 0), (0, 0, 1), (0, 2, 0), (0, 1, 1), (0, 1, 2), (0, 4, 0), (0, 0, 2), (0, 0, 3), (0, 3, 0),
    (1, 0, 0), (5, 0, 0), (5, 1, 0), (0, 2, 1), (1, 2, 0), (4, 0, 0), (4, 1, 0), (1, 1, 0), (2, 0, 0), (2, 0, 1),
    (0, 3, 1), (2, 1, 0), (0, 3, 2), (5, 2, 0), (2, 3, 0), (0, 2, 2), (4, 2, 0), (5, 3, 0), (4, 3, 0), (0, 4, 1),
    (2, 2, 0), (2, 3, 1), (1, 3, 0), (2, 1, 1), (2, 0, 2), (0, 3, 3), (2, 2, 1), (1, 0, 1), (1, 3, 1), (1, 1, 1),
    (1, 2, 1), (0, 4, 2), (5, 4, 0), (0, 1, 3), (5, 5, 0), (2, 3, 2), (4, 4, 0), (3, 1, 0), (2, 0, 3), (4, 5, 0),
    (3, 0, 0), (2, 5, 0), (1, 0, 2), (2, 1, 2), (2, 2, 2), (2, 7, 0), (2, 6, 0), (3, 3, 0), (1, 1, 2), (2, 4, 0),
    (2, 1, 3), (3, 1, 1), (5, 6, 0), (4, 6, 0), (3, 3, 1), (2, 3, 3), (2, 5, 1), (2, 2, 3), (3, 2, 0), (2, 6, 1),
    (1, 3, 2), (1, 2, 2), (2, 7, 1), (0, 2, 3), (0, 4, 3), (2, 5, 2), (3, 0, 1), (3, 1, 2), (3, 5, 0), (2, 7, 2),
    (3, 2, 1), (3, 4, 0), (3, 6, 0), (3, 4, 1), (3, 7, 0), (2, 4, 1), (3, 5, 1), (3, 6, 1), (3, 3, 2), (1, 1, 3),
    (2, 6, 2), (2, 7, 3), (1, 0, 3), (2, 5, 3), (3, 4, 2), (3, 7, 1), (3, 2, 2), (2, 4, 2), (3, 7, 2), (1, 3, 3),
    (3, 6, 2), (3, 5, 2), (3, 0, 2), (2, 6, 3), (3, 0, 3), (3, 1, 3), (3, 3, 3), (3, 2, 3), (1, 2, 3), (3, 5, 3),
    (2, 4, 3), (3, 7, 3), (3, 6, 3), (3, 4, 3),
)
FLAT = (
    (0, 0), (1, 2), (2, 1), (2, 4), (3, 0),
)
PAIRED = (
    (0, 3), (1, 1), (2, 0), (2, 2), (2, 3), (2, 6), (3, 1), (3, 2), (3, 5), (3, 7),
)
PAIR_SENT = (-1, -1, -1, -2)
SUBS = 4
OWN_CHUNK = (0, 0, 1, 1, 1)
OWN_ROW = ((0, 2, 1, 0, 3), (2, 1, 3, 2, 0))


def plain(slabs, significant):
    aux_here, occupied, rows_here = slabs.shape
    blocks_here = rows_here // BS
    first_block = lax.axis_index("row") * blocks_here
    local_mask = lax.dynamic_slice_in_dim(significant, first_block, blocks_here, 1).astype(
        jnp.float32
    )
    block_of = lax.broadcasted_iota(jnp.int32, (blocks_here, rows_here), 1) // BS
    block_id = lax.broadcasted_iota(jnp.int32, (blocks_here, rows_here), 0)
    expand_table = (block_of == block_id).astype(jnp.float32)
    column_mask = jnp.dot(local_mask, expand_table).astype(jnp.bfloat16)
    masked = (slabs * column_mask[:, None, :]).reshape(aux_here * occupied, rows_here)
    partial_rows = lax.dot_general(
        masked,
        lax.all_gather(masked, "row", axis=1, tiled=True),
        (((0,), (0,)), ((), ())),
        preferred_element_type=jnp.float32,
    )
    return lax.psum_scatter(partial_rows, "aux", scatter_dimension=1, tiled=True)


def kernel(n_aux, n_row, occupied, slab_hbm, sig, out_ref, g, gy, lhs_t, mk, mkc, mask_ref, psd, pso, psc,
           xr, zb, zl, nb, mr, own_sem, psend, precv, ysend, yrecv, fsend, frecv, xsend, xrecv,
           zsend, zrecv, nsend, nrecv, msend, mrecv, go):
    depth = slab_hbm.shape[0]
    half = depth // 2
    aux_here = depth // occupied
    width = CHUNKS * LANES
    a, r = lax.axis_index("aux"), lax.axis_index("row")
    z, x = a // 2, a % 2
    last = n_aux // 2 - 1
    y, c = r // 2, r % 2
    partner = y * 2 + (1 - c)
    across = (1 - y) * 2 + c
    beside = z * 2 + (1 - x)
    over = ((1 - y) * 2 + (1 - y), (1 - y) * 2 + y)
    direct = jnp.where(c == y, 1, 0)
    sent = 1 - direct

    barrier = pltpu.get_barrier_semaphore()
    for there in ({"row": partner}, {"row": across}, {"aux": beside},
                  *({"aux": lax.rem(a + 2 * n, n_aux)} for n in range(1, n_aux // 2))):
        pl.semaphore_signal(barrier, inc=1, device_id=there, device_id_type=pl.DeviceIdType.MESH)

    def greet(*theirs):
        for there in theirs:
            pl.semaphore_signal(barrier, inc=1, device_id=there, device_id_type=pl.DeviceIdType.MESH)

    pl.when(z != r)(lambda: greet(*({"aux": r * 2 + q, "row": z} for q in range(2))))

    @pl.when(z == r)
    def _():
        greet(*({"aux": r * 2 + q, "row": d} for q in range(2) for d in over))

    @pl.when((z != r) & (z != partner))
    def _():
        greet(*({"aux": z * 2 + q, "row": z} for q in range(2)))

    def lanes(h, j):
        return pl.ds(pl.multiple_of(h * width + j * LANES, LANES), LANES)

    def piece(j, h):
        return slab_hbm.at[:, lanes(h, j)]

    def remote(src, dst, send, recv, there):
        return pltpu.make_async_remote_copy(
            src_ref=src, dst_ref=dst, send_sem=send, recv_sem=recv, device_id=there,
            device_id_type=pl.DeviceIdType.MESH,
        )

    both = [(j, h) for j in range(CHUNKS) for h in range(2)]
    own = {w: pltpu.make_async_copy(piece(*w), g.at[(0,) + w], own_sem.at[w]) for w in both}
    for w in both:
        own[w].start()

    low_lanes = lax.broadcasted_iota(jnp.int32, (16, LANES), 1) < BS
    for q in range(aux_here):
        for d in range(n_row):
            for h in range(2):
                for j in range(CHUNKS):
                    b = (d * 2 * width + h * width + j * LANES) // BS
                    tile = jnp.where(low_lanes, sig[q, b], sig[q, b + 1])
                    mask_ref[d, h, j, q] = tile.astype(jnp.float32).astype(jnp.bfloat16)

    pl.semaphore_wait(barrier, jnp.where(z == partner, 8, 10))

    def side(i):
        return x if i else 1 - x

    def y_copy(j, i):
        first = pl.multiple_of((1 - y) * half, 16)
        return remote(slab_hbm.at[pl.ds(first, half), lanes(side(i), j)], gy.at[sent, j, i],
                      ysend.at[j, i], yrecv.at[j, i], {"row": across})

    def f_copy(q, j, i):
        return remote(gy.at[q, j, i], gy.at[q, j, i], fsend.at[j, i], frecv.at[j, i], {"row": partner})

    to_p = {w: remote(piece(*w), g.at[(1,) + w], psend.at[w], precv.at[w], {"row": partner}) for w in both}

    @pl.when(c == y)
    def _():
        for w in both:
            y_copy(*w).start()

    for w in both:
        to_p[w].start()

    def apply(raw, mask):
        return (raw.reshape(-1, occupied // 16, 16, LANES) * mask[:, None]).reshape(raw.shape)

    count = (len(OWN_CHUNK), SUBS, CHUNKS * SUBS, CHUNKS * SUBS)
    base = [sum(count[:k]) for k in range(4)]

    def turned(kind, i):
        return (kind, i) in TURNED

    def dest(kind, i):
        return r if kind == OWN or turned(kind, i) else partner if kind == PAIR else over[kind - FIRST]

    def rows_of(s):
        return pl.ds(s * SUB, SUB) if isinstance(s, int) else pl.ds(pl.multiple_of(s * SUB, SUB), SUB)

    def partial_tile(kind, i, there):
        if kind == OWN:
            s = jnp.where((x if not there else 1 - x) == 0, OWN_ROW[0][i], OWN_ROW[1][i])
            return psd.at[OWN_CHUNK[i], 1 - x if there else x, rows_of(s)]
        if kind == PAIR:
            return pso.at[1 - x if there else x, rows_of(i)]
        return psc.at[kind - FIRST, i // SUBS, 0 if there else 1, rows_of(i % SUBS)]

    def x_copy(kind, i):
        e = base[kind] + i
        return remote(partial_tile(kind, i, True), xr.at[e], xsend.at[e], xrecv.at[e], {"aux": beside})

    def parent(kind, i):
        d = dest(kind, i)
        near = jnp.where(z < d, z + 1, z - 1)
        if (kind, i) in FLAT:
            return d
        if (kind, i) in PAIRED:
            return jnp.where((d == 0) & (z == 2) | (d == last) & (z == 1), d, near)
        return near

    def z_copy(kind, i):
        e = base[kind] + i
        return remote(zb.at[e], zl.at[e, z], zsend.at[e], zrecv.at[e, z], {"aux": parent(kind, i) * 2 + x})

    def add_from(kind, i, child):
        e = base[kind] + i
        remote(zb.at[e], zl.at[e, child], zsend.at[e], zrecv.at[e, child], {"aux": beside}).wait_recv()
        zb[e] += zl[e, child]

    def level(kind, i):
        d = dest(kind, i)
        if (kind, i) in FLAT:
            return jnp.where(z == d, 1, 0)
        line = jnp.where(z < d, z, jnp.where(z > d, last - z, jnp.maximum(d, last - d)))
        if (kind, i) in PAIRED:
            inner = jnp.where((z == 0) | (z == last) | (jnp.abs(z - d) == 1), 0, 1)
            return jnp.where((d == 0) | (d == last), jnp.where(z == d, 2, inner), line)
        return line

    def m_copy(kind, i):
        e = base[kind] + i
        if kind == OWN:
            slot = 0 if i == 1 else 1
            return remote(zb.at[e], mr.at[slot, 0], msend.at[e], mrecv.at[slot, 0], {"aux": beside})
        s = i % SUBS
        j = (s + c) % 2 if kind == PAIR else i // SUBS
        to = x * CHUNKS + j
        return remote(zb.at[e], mr.at[s % CHUNKS, to], msend.at[e], mrecv.at[s % CHUNKS, to],
                      {"aux": r * 2 + s // CHUNKS, "row": partner if kind == PAIR else over[kind - FIRST]})

    def n_copy(kind, i):
        e = (kind - FIRST) * CHUNKS * SUBS + i
        return remote(zb.at[base[kind] + i], nb.at[e], nsend.at[e], nrecv.at[e], {"aux": over[kind - FIRST] * 2 + x})

    def sum_x(kind, i):
        e = base[kind] + i
        x_copy(kind, i).wait_recv()
        zb[e] = partial_tile(kind, i, False)[...] + xr[e]
        pl.when(level(kind, i) == 0)(lambda: z_copy(kind, i).start())

    def finish(kind, i, hop):
        e = base[kind] + i
        if kind == OWN:
            j = OWN_CHUNK[i]
            for side_x in range(2):
                @pl.when(x == side_x)
                def _():
                    s = OWN_ROW[side_x][i]
                    out_ref[s * SUB:(s + 1) * SUB, j * LANES:(j + 1) * LANES] = zb[e]
                    if i == 3:
                        t = side_x * CHUNKS + j
                        u = (s % CHUNKS) * LANES
                        out_ref[t * SUB:(t + 1) * SUB, u:u + LANES] = zb[e].T
            if i in (1, 4):
                m_copy(kind, i).start()
        elif kind == PAIR:
            m_copy(kind, i).start()
            for core in range(2):
                @pl.when(c == core)
                def _():
                    j = (i + core) % 2
                    out_ref[i * SUB:(i + 1) * SUB, j * LANES:(j + 1) * LANES] = zb[e]
        else:
            if turned(kind, i):
                n_copy(kind, i).start()
            if late[0] or (kind, i) not in HELD:
                m_copy(kind, i).start()
            else:
                held.append((kind, i, hop))

    def sum_z(kind, i, hop):
        d = dest(kind, i)
        if (kind, i) in FLAT:
            for away in range(1, last + 1):
                add_from(kind, i, lax.rem(z + away, last + 1))
        elif (kind, i) in PAIRED:
            ends = (d == 0) | (d == last)
            far = jnp.where(z == d, jnp.where(d == 0, 2, 1), jnp.where(d == 0, last, 0))
            pl.when(ends)(lambda: add_from(kind, i, far))
            pl.when(ends & (z == d))(lambda: add_from(kind, i, jnp.where(d == 0, 1, last - 1)))
            pl.when(~ends & (z > 0) & (z <= d))(lambda: add_from(kind, i, z - 1))
            pl.when(~ends & (z < last) & (z >= d))(lambda: add_from(kind, i, z + 1))
        else:
            pl.when((z > 0) & (z <= d))(lambda: add_from(kind, i, z - 1))
            pl.when((z < last) & (z >= d))(lambda: add_from(kind, i, z + 1))
        pl.when(z != d)(lambda: z_copy(kind, i).start())
        pl.when(z == d)(lambda: finish(kind, i, hop))

    late, held = [False], []

    def pull(q, j, i):
        @pl.when(direct == q)
        def _():
            remote(gy.at[q, j, i], gy.at[q, j, i], ysend.at[j, i], yrecv.at[j, i], {"row": across}).wait_recv()
            f_copy(q, j, i).start()

    def product(q, j, i):
        pl.when(direct != q)(lambda: f_copy(q, j, i).wait_recv())
        here = half // occupied
        mkc[...] = apply(gy[q, j, i], mask_ref[over[q], side(i), j, pl.ds(y * here, here)])
        for s in range(0, SUBS, 2):
            part = slice(s * SUB, (s + 2) * SUB)
            psc[q, j, i, part, :] = jnp.dot(lhs_t[y, part, :], mkc[...], preferred_element_type=jnp.float32)
        if i == 0:
            for s in range(SUBS):
                x_copy(FIRST + q, j * SUBS + s).start()

    for j, h in both:
        own[j, h].wait()
        mk[j, :, h * LANES:(h + 1) * LANES] = apply(g[0, j, h], mask_ref[r, h, j])
        for e in range(2):
            t = h * CHUNKS + j
            lhs_t[e, t * LANES:(t + 1) * LANES, :] = mk[j, e * half:(e + 1) * half, h * LANES:(h + 1) * LANES].T
    for j in range(CHUNKS):
        for s in range(0, SUBS, 2):
            part = slice(s * SUB, (s + 2) * SUB)
            acc = jnp.dot(lhs_t[0, part, :], mk[j, :half, :], preferred_element_type=jnp.float32)
            acc += jnp.dot(lhs_t[1, part, :], mk[j, half:, :], preferred_element_type=jnp.float32)
            psd[j, 0, part, :] = acc[:, :LANES]
            psd[j, 1, part, :] = acc[:, LANES:]
        for i in range(len(OWN_CHUNK)):
            if OWN_CHUNK[i] == j:
                x_copy(OWN, i).start()

    @pl.when(c == y)
    def _():
        y_copy(0, 0).wait_send()
        pl.semaphore_signal(go, inc=1, device_id={"row": partner}, device_id_type=pl.DeviceIdType.MESH)

    @pl.when(c != y)
    def _():
        pl.semaphore_wait(go, 1)
        for w in ((0, 0), (1, 0), (0, 1), (1, 1)):
            y_copy(*w).start()

    pull(0, 0, 0)
    for j, h in both:
        to_p[j, h].wait_recv()
        mk[j, :, h * LANES:(h + 1) * LANES] = apply(g[1, j, h], mask_ref[partner, h, j])
    for s in range(SUBS):
        part = slice(s * SUB, (s + 1) * SUB)
        j = (s + c) % 2
        acc = jnp.dot(lhs_t[0, part, :], mk[j, :half, :], preferred_element_type=jnp.float32)
        acc += jnp.dot(lhs_t[1, part, :], mk[j, half:, :], preferred_element_type=jnp.float32)
        pso[0, part, :] = acc[:, :LANES]
        pso[1, part, :] = acc[:, LANES:]
        if PAIR_SENT[s] == -1:
            x_copy(PAIR, s).start()
    product(0, 0, 0)
    for s in range(SUBS):
        if PAIR_SENT[s] == -2:
            x_copy(PAIR, s).start()

    order = [(q, j) for j in range(CHUNKS) for q in range(2)]

    groups = [(order[1], 0), (order[0], 1), (order[2], 0), (order[3], 0), (order[1], 1), (order[2], 1), (order[3], 1)]

    def step(n):
        product(*groups[n][0], groups[n][1])
        for p in range(SUBS):
            if PAIR_SENT[p] == n:
                x_copy(PAIR, p).start()

    def release():
        for kind, i, hop in held:
            d = dest(kind, i)
            pl.when((z == d) & (level(kind, i) == hop))(lambda: m_copy(kind, i).start())
        late[0] = True

    for kind, i, hop in ORDER:
        if kind == PULL:
            pull(*groups[i][0], groups[i][1])
        elif kind == PIECES:
            step(i)
            if i == len(groups) - 1:
                release()
        elif hop == 0:
            sum_x(kind, i)
        else:
            pl.when(level(kind, i) == hop)(functools.partial(sum_z, kind, i, hop))

    @pl.when(z == r)
    def _():
        for slot in range(2):
            m_copy(OWN, 1 + 3 * slot).wait_recv()
            for side_x in range(2):
                @pl.when(x == side_x)
                def _():
                    s, t = OWN_ROW[1 - side_x][1 + 3 * slot], (1 - side_x) * CHUNKS + OWN_CHUNK[1 + 3 * slot]
                    u = (s % CHUNKS) * LANES
                    out_ref[t * SUB:(t + 1) * SUB, u:u + LANES] = mr[slot, 0].T
        for slot in range(2):
            m_copy(OWN, 1 + 3 * slot).wait_send()

    def landed(j, t):
        remote(mr.at[j, t], mr.at[j, t], msend.at[0], mrecv.at[j, t], {"aux": r * 2, "row": z}).wait_recv()

    for core in range(2):
        @pl.when((z == partner) & (c == core))
        def _():
            for t in range(SUBS):
                j = 1 - (t + core) % 2
                landed(j, t)
                out_ref[t * SUB:(t + 1) * SUB, j * LANES:(j + 1) * LANES] = mr[j, t].T
            for s in range(SUBS):
                m_copy(PAIR, s).wait_send()

    for q in range(2):
        @pl.when(z == over[q])
        def _():
            for j_from in range(CHUNKS):
                for j in range(CHUNKS):
                    for t in range(j_from, SUBS, CHUNKS):
                        i = j * SUBS + t
                        if turned(FIRST + q, i):
                            n_copy(FIRST + q, i).wait_recv()
                            mine = nb.at[q * CHUNKS * SUBS + i]
                        else:
                            mine = zb.at[base[FIRST + q] + i]
                        landed(j, t)
                        out_ref[t * SUB:(t + 1) * SUB, j * LANES:(j + 1) * LANES] = mine[...] + mr[j, t].T

        for i in range(CHUNKS * SUBS):
            @pl.when(z == dest(FIRST + q, i))
            def _():
                m_copy(FIRST + q, i).wait_send()
                if turned(FIRST + q, i):
                    n_copy(FIRST + q, i).wait_send()

    pl.when(c != y)(lambda: y_copy(0, 0).wait_send())
    for w in both:
        if w != (0, 0):
            y_copy(*w).wait_send()
        to_p[w].wait_send()
        f_copy(direct, *w).wait_send()
    for kind in range(4):
        for i in range(count[kind]):
            x_copy(kind, i).wait_send()
            pl.when(z != dest(kind, i))(lambda: z_copy(kind, i).wait_send())


def solution(mesh):
    n_aux, n_row = mesh.shape["aux"], mesh.shape["row"]

    def local(slabs, significant):
        aux_here, occupied, rows = slabs.shape
        nbf = rows * n_row
        cols = nbf // n_aux
        fits = (n_row == 4 and n_aux == 2 * n_row and cols == CHUNKS * LANES and rows == SUBS * SUB
                and occupied % 16 == 0 and aux_here % 2 == 0 and LANES == 2 * BS)
        if not fits:
            return plain(slabs, significant)
        depth = aux_here * occupied
        items = len(OWN_CHUNK) + SUBS + 2 * CHUNKS * SUBS
        dma = pltpu.SemaphoreType.DMA
        tile = pltpu.VMEM((items, SUB, LANES), jnp.float32)
        return pl.pallas_call(
            functools.partial(kernel, n_aux, n_row, occupied),
            out_shape=jax.ShapeDtypeStruct((rows, cols), jnp.float32),
            in_specs=[pl.BlockSpec(memory_space=pl.ANY), pl.BlockSpec(memory_space=pltpu.SMEM)],
            out_specs=pl.BlockSpec(memory_space=pltpu.VMEM),
            scratch_shapes=[
                pltpu.VMEM((2, CHUNKS, 2, depth, LANES), jnp.bfloat16),
                pltpu.VMEM((2, CHUNKS, 2, depth // 2, LANES), jnp.bfloat16),
                pltpu.VMEM((2, rows, depth // 2), jnp.bfloat16),
                pltpu.VMEM((CHUNKS, depth, 2 * LANES), jnp.bfloat16),
                pltpu.VMEM((depth // 2, LANES), jnp.bfloat16),
                pltpu.VMEM((n_row, 2, CHUNKS, aux_here, 16, LANES), jnp.bfloat16),
                pltpu.VMEM((CHUNKS, 2, rows, LANES), jnp.float32),
                pltpu.VMEM((2, rows, LANES), jnp.float32),
                pltpu.VMEM((2, CHUNKS, 2, rows, LANES), jnp.float32),
            ]
            + [tile] * 2
            + [pltpu.VMEM((items, n_aux // 2, SUB, LANES), jnp.float32)]
            + [pltpu.VMEM((2 * CHUNKS * SUBS, SUB, LANES), jnp.float32)]
            + [pltpu.VMEM((CHUNKS, SUBS, SUB, LANES), jnp.float32)]
            + [dma((CHUNKS, 2))] * 7
            + [dma((items,))] * 3
            + [dma((items, n_aux // 2))]
            + [dma((2 * CHUNKS * SUBS,))] * 2
            + [dma((items,)), dma((CHUNKS, SUBS))]
            + [pltpu.SemaphoreType.REGULAR],
            compiler_params=pltpu.CompilerParams(
                collective_id=0, has_side_effects=True, vmem_limit_bytes=60 * 2**20
            ),
            cost_estimate=pl.CostEstimate(
                flops=2 * rows * nbf * depth, bytes_accessed=2 * depth * rows, transcendentals=0
            ),
        )(slabs.reshape(depth, rows), significant)

    return jax.shard_map(
        local,
        mesh=mesh,
        in_specs=(P("aux", None, "row"), P("aux", None)),
        out_specs=P("row", "aux"),
        check_vma=False,
    )
```
